32 devices in a mesh: row: 8 (over y, x, core), col: 4 (over z).
Axes of the slice: x: 2, y: 2, z: 4, core: 2. Of those that a mesh axis runs over, the one named last changes fastest.
Arguments:
- tokens: bfloat16 [256, 7168], P(('row', 'col')), may hold values from -6 to 6
- router_logits: float32 [256, 16], P(('row', 'col')), may hold values from -18 to 318
- expert_ids: int32 [256, 8], P(('row', 'col')), may hold values from 0 to 15, all different within a row; in each aligned block of 8 rows (0 to 7, 8 to 15, ...) at most 8 rows name the same one
- w_gate: bfloat16 [16, 7168, 2048], P('row', None, 'col'), may hold values from -0.3307189 to 0.3307189
- w_up: bfloat16 [16, 7168, 2048], P('row', None, 'col'), may hold values from -0.3307189 to 0.3307189
- w_down: bfloat16 [16, 2048, 7168], P('row', 'col'), may hold values from -0.61871843 to 0.61871843
Outputs:
- merged: bfloat16 [256, 7168], P(('row', 'col'))
The draws below stay inside these ranges and needn't reach their ends.
Inputs may be any that keep to these rules, and one draw needn't show every extreme that they name: `expert_ids`: each row names 8 different experts. Among the 8 tokens of one device no expert is named more than 8 times, and in every draw some device names some expert exactly 8 times.
All inputs are finite; a program needn't handle non-finite values.
Results may differ from the reference program's by a relative error of at most 0.015.
Values may be sent and summed in bfloat16 or wider, within the bound.
A program may use at most 128 MiB of HBM per device.

```python
import math
import jax
import jax.numpy as jnp
import numpy as np
from jax import lax

D = 7168
FF = 2048
TOP = 8
EXP_ROW = 2
TOK_DEV = 8
EXPERTS = 16
TOKENS = 256
CAP = 8
N_ROW = 8
N_COL = 4


def expert_levels(key):
    groups = EXPERTS // EXP_ROW
    count = max(1, groups // 4)
    order = jax.random.permutation(jax.random.fold_in(key, 5), groups)
    group_flags = (order < count).astype(jnp.float32)
    return jnp.repeat(group_flags, EXP_ROW)


def scaled_weight(key, salt, shape, fan_in):
    flags = expert_levels(key)
    factor = 1.0 + 7.0 * flags
    values = jnp.clip(jax.random.normal(jax.random.fold_in(key, salt), shape, jnp.float32), -3.5, 3.5)
    values = values * factor[:, None, None] * fan_in ** (-0.5)
    return values.astype(jnp.bfloat16)


def draw_router_logits(key, part):
    first = jax.random.fold_in(key, 11)
    flags = expert_levels(key)
    noise = jax.random.normal(first, (TOKENS, EXPERTS), jnp.float32)
    base = jnp.where(flags[None, :] > 0.5, -4.5 + 0.5 * noise, 1.5 * noise)
    base = jnp.clip(base, -18.0, 18.0)
    return base


def draw_w_gate(key, part):
    return scaled_weight(key, 21, (EXPERTS, D, FF), D)


def draw_w_up(key, part):
    return scaled_weight(key, 22, (EXPERTS, D, FF), D)


def draw_w_down(key, part):
    return scaled_weight(key, 23, (EXPERTS, FF, D), FF)


def levels(stream_key, dims, cuts, smallest, high):
    def one(dim, blocks):
        draws = jax.random.uniform(jax.random.fold_in(jax.random.fold_in(stream_key, 6), dim), (blocks,), jnp.float32, smallest / len(cuts), high / len(cuts))
        return jnp.repeat(jnp.exp(draws), dims[dim] // blocks).reshape((-1,) + (1,) * (len(dims) - dim - 1))

    level = one(*cuts[0])
    for cut in cuts[1:]:
        level = level * one(*cut)
    return level


def deal_out(stream_key, own, number, rows, amount, top, most, lean):
    sequence = jax.random.permutation(stream_key, amount)
    packed, common = portions_of(amount, rows * top, most, lean, True), portions_of(amount, rows * top, most, lean, False)
    places = jnp.arange(amount)

    def named(sizes, offset_by):
        used = int((sizes > 0).sum())
        fixed = max(1, used // 4)
        moved = fixed + (places - fixed + offset_by * (used - fixed)) % max(1, amount - fixed)
        return jnp.zeros((amount,), jnp.int32).at[sequence[jnp.where(places < fixed, places, moved)]].set(jnp.asarray(sizes, jnp.int32))

    sizes = jnp.where(number % 4 == 0, named(packed, number // 4), named(common, number - number // 4 - 1))
    mixed = jax.random.permutation(jax.random.fold_in(own, 3), amount)
    giver, receiver = mixed[0:amount // 2 * 2:2], mixed[1:amount // 2 * 2:2]
    slack = jnp.minimum(sizes[giver] - 1, most - sizes[receiver]) // 2
    slack = jnp.where((giver == sequence[0]) | (receiver == sequence[0]) | (sizes[receiver] == 0), 0, jnp.maximum(slack, 0))
    moved = jax.random.randint(jax.random.fold_in(own, 4), (amount // 2,), 0, 1 << 20) % (slack + 1)
    sizes = sizes.at[giver].add(-moved).at[receiver].add(moved)
    members = jnp.searchsorted(jnp.cumsum(sizes), jnp.arange(rows * top), side="right").astype(jnp.int32)
    listing = members.reshape(top, rows).T
    listing = listing[jax.random.permutation(jax.random.fold_in(own, 1), rows)]
    offset_by = jax.random.randint(jax.random.fold_in(own, 2), (rows, 1), 0, top)
    return jnp.take_along_axis(listing, (jnp.arange(top)[None, :] + offset_by) % top, axis=1)


def portions_of(number_of, total, bound, slope, full):
    portions = [(1 << 20) // math.isqrt(grade ** slope) + 1 for grade in range(1, number_of + 1)]
    largest = bound if full else min(bound, max(-(-total // number_of), total * portions[0] // sum(portions)))
    least = 1 if total - largest >= number_of - 1 else 0
    counts, surplus = [largest] + [least] * (number_of - 1), total - largest - least * (number_of - 1)
    while surplus > 0:
        free = [i for i in range(1, number_of) if counts[i] < largest] or [i for i in range(1, number_of) if counts[i] < bound]
        pool, left = sum([portions[i] for i in free]), surplus
        for i in free:
            extra = min(bound - counts[i], max(1, left * portions[i] // pool), surplus)
            counts[i] = counts[i] + extra
            surplus = surplus - extra
    return np.array(counts)


def scatter_about(rng, dims, deviation, bound, shards=(), kind=jnp.bfloat16):
    array = deviation * jax.random.normal(rng, dims, jnp.float32)
    if shards:
        array = array * levels(rng, dims, shards, -0.22, 0.18)
    return jnp.clip(array, -bound, bound).astype(kind)


def setup_inputs(seed: int = 0) -> dict:
    keys = jax.random.split(jax.random.key(seed), 7)
    tokens = scatter_about(keys[0], (TOKENS, D), 1.0, 6.0, ((0, 32),))
    router_logits = draw_router_logits(jax.random.fold_in(keys[6], 71), 0)
    expert_ids_keys = jax.random.split(jax.random.fold_in(keys[2], 1), TOKENS // TOK_DEV)
    expert_ids_turns = jax.random.permutation(jax.random.fold_in(keys[2], 3), TOKENS // TOK_DEV)
    expert_ids = jax.vmap(lambda own, number: deal_out(jax.random.fold_in(keys[2], 2), own, number, TOK_DEV, EXPERTS, TOP, CAP, 2))(expert_ids_keys, expert_ids_turns).reshape((TOKENS, TOP))
    w_gate = draw_w_gate(jax.random.fold_in(keys[6], 71), 0)
    w_up = draw_w_up(jax.random.fold_in(keys[6], 71), 0)
    w_down = draw_w_down(jax.random.fold_in(keys[6], 71), 0)
    return dict(tokens=tokens, router_logits=router_logits, expert_ids=expert_ids, w_gate=w_gate, w_up=w_up, w_down=w_down)


def reference(tokens, router_logits, expert_ids, w_gate, w_up, w_down):
    picked = jnp.take_along_axis(router_logits, expert_ids, axis=1)
    probs = lax.optimization_barrier(jax.nn.softmax(picked, axis=-1).astype(jnp.bfloat16)).astype(jnp.float32)
    marks = expert_ids[:, :, None] == jnp.arange(EXPERTS, dtype=jnp.int32)[None, None, :]
    table = jnp.sum(probs[:, :, None] * marks.astype(jnp.float32), axis=1)
    picks = jnp.any(marks, axis=1).astype(jnp.int32)
    slice_width = FF // N_COL
    per_group = EXPERTS // N_ROW
    limit = min(TOKENS, CAP * N_ROW * N_COL)

    def group_sum(total, group):
        terms = jnp.zeros((N_COL, TOKENS, D), jnp.float32)
        for inner in range(per_group):
            expert = group * per_group + inner
            flags = lax.dynamic_index_in_dim(picks, expert, 1, keepdims=False)
            order = jnp.argsort(1 - flags, stable=True)[:limit].astype(jnp.int32)
            chosen_rows = tokens[order]
            gate = jnp.dot(chosen_rows, w_gate[expert], preferred_element_type=jnp.float32)
            up = jnp.dot(chosen_rows, w_up[expert], preferred_element_type=jnp.float32)
            hidden = (jax.nn.silu(gate) * up).astype(jnp.bfloat16)
            sliced = hidden.astype(jnp.float32).reshape(limit, N_COL, slice_width)
            down = w_down[expert].astype(jnp.float32).reshape(N_COL, slice_width, D)
            outputs = jnp.einsum("tcf,cfd->ctd", sliced, down, precision=lax.Precision.HIGHEST)
            weight = lax.dynamic_index_in_dim(table, expert, 1, keepdims=False)[order]
            terms = terms.at[:, order].add(outputs * weight[None, :, None])
        rounded = lax.optimization_barrier(terms.astype(jnp.bfloat16)).astype(jnp.float32)
        group_out = lax.optimization_barrier(jnp.sum(rounded, axis=0).astype(jnp.bfloat16)).astype(jnp.float32)
        return total + group_out, None

    total, _ = lax.scan(group_sum, jnp.zeros((TOKENS, D), jnp.float32), jnp.arange(N_ROW, dtype=jnp.int32))
    return total.astype(jnp.bfloat16)
```

```python
import functools
import jax
import jax.numpy as jnp
from jax import lax
from jax.experimental import pallas as pl
from jax.experimental.pallas import tpu as pltpu
from jax.sharding import PartitionSpec as P

MESH = pl.DeviceIdType.MESH
LANES = 128


def column_chunks(width, wanted):
    tiles = width // LANES
    count = max(n for n in range(1, wanted + 1) if tiles % n == 0)
    return count, width // count


def split_parts(width, count):
    tiles = width // LANES
    edges = [tiles * i // count * LANES for i in range(count + 1)]
    return [(edges[i], edges[i + 1] - edges[i]) for i in range(count)]


class Copies:
    def __init__(self, send_sems, recv_sems):
        self.send_sems, self.recv_sems, self.used, self.sent = send_sems, recv_sems, 0, []

    def start(self, src, dst, target):
        n = self.used
        self.used += 1
        copy = pltpu.make_async_remote_copy(
            src_ref=src,
            dst_ref=dst,
            send_sem=self.send_sems.at[n],
            recv_sem=self.recv_sems.at[n],
            device_id=target,
            device_id_type=MESH,
        )
        copy.start()
        self.sent.append(copy)
        return copy


def kernel(
    n_row, n_col, count, chunk,
    tokens_hbm, logits_hbm, ids_hbm, gate_hbm, up_hbm, down_hbm,
    out_ref,
    tok, logits, ids, table_own, wg, wu, wd,
    zbuf, ztab, xbuf, xtab, acc, hid, part, rcore, rstage, p3, r4,
    small_sems, weight_sems, send_sems, recv_sems,
):
    bits = n_row.bit_length() - 1
    upper = list(range(1, bits))
    tok_count = tok.shape[0]
    rows = n_col * tok_count
    per_group, ff = wg.shape[1], wg.shape[3]
    total = n_row * rows
    experts = logits.shape[1]

    row, col = lax.axis_index("row"), lax.axis_index("col")
    mine = [(row // 2**i) % 2 for i in range(bits)]

    def across(i):
        return {"row": row + 2**i * (1 - 2 * mine[i]), "col": col}

    def along(j):
        return {"row": row, "col": (col + j) % n_col}

    def at(fixed, *tail):
        return tuple(fixed.get(i, slice(None)) for i in reversed(range(bits))) + (slice(None),) + tail

    orders = [upper[p:] + upper[:p] for p in range(len(upper))]

    small = [
        pltpu.make_async_copy(src, dst, small_sems.at[i])
        for i, (src, dst) in enumerate(((tokens_hbm, tok), (logits_hbm, logits), (ids_hbm, ids)))
    ]
    for copy in small:
        copy.start()
    gate_up, down = [], []
    for c in range(count):
        span = pl.ds(c * chunk, chunk)
        pair = [
            pltpu.make_async_copy(gate_hbm.at[:, span, :], wg.at[c], weight_sems.at[0, c]),
            pltpu.make_async_copy(up_hbm.at[:, span, :], wu.at[c], weight_sems.at[1, c]),
        ]
        for copy in pair:
            copy.start()
        gate_up.append(pair)
    for c in range(count):
        copy = pltpu.make_async_copy(down_hbm.at[:, :, pl.ds(c * chunk, chunk)], wd.at[c], weight_sems.at[2, c])
        copy.start()
        down.append(copy)

    barrier = pltpu.get_barrier_semaphore()
    peers = [across(i) for i in range(bits)] + [along(j) for j in range(1, n_col)]
    for peer in peers:
        pl.semaphore_signal(barrier, inc=1, device_id=peer, device_id_type=MESH)

    small[1].wait()
    small[2].wait()
    scores, named = logits[...], ids[...]
    lane = lax.broadcasted_iota(jnp.int32, scores.shape, 1)
    marks = jnp.zeros(scores.shape, jnp.float32)
    for k in range(named.shape[1]):
        marks = marks + jnp.where(named[:, k : k + 1] == lane, 1.0, 0.0)
    chosen = marks > 0.5
    top = jnp.max(jnp.where(chosen, scores, -jnp.inf), axis=1, keepdims=True)
    weight = jnp.where(chosen, jnp.exp(jnp.where(chosen, scores, top) - top), 0.0)
    weight = weight / jnp.sum(weight, axis=1, keepdims=True)
    table_own[...] = jnp.zeros(table_own.shape, table_own.dtype)
    table_own[:, :experts] = weight.astype(table_own.dtype)
    small[0].wait()

    pl.semaphore_wait(barrier, len(peers))
    copies = Copies(send_sems, recv_sems)

    parts = split_parts(chunk, len(upper))
    pieces = [(table_own, ztab, xtab, [(0, LANES)])]
    pieces += [(tok.at[:, pl.ds(c * chunk, chunk)], zbuf.at[c], xbuf.at[c], parts) for c in range(count)]
    flights = []
    for own, z, _, _ in pieces:
        flights.append([copies.start(own, z.at[col], along(j)) for j in range(1, n_col)])
        z[col] = own[...]

    def gather_first(n):
        own, z, x, spans = pieces[n]
        for copy in flights[n]:
            copy.wait_recv()
        block = z[...].astype(jnp.float32).reshape(rows, z.shape[-1]).astype(x.dtype)
        x[at({i: mine[i] for i in range(bits)}, slice(None))] = block
        gather_stage(n, 0)

    def gather_stage(n, k):
        _, _, x, spans = pieces[n]
        flights[n] = []
        for p, (offset, width) in enumerate(spans):
            done = orders[p][:k]
            fixed = {i: mine[i] for i in range(bits) if i not in done}
            view = x.at[at(fixed, pl.ds(offset, width))]
            flights[n].append(copies.start(view, view, across(orders[p][k])))

    def gather_next(n, k):
        for copy in flights[n]:
            copy.wait_recv()
        if k < len(upper):
            gather_stage(n, k)
        else:
            _, _, x, _ = pieces[n]
            view = x.at[at({0: mine[0]}, slice(None))]
            flights[n] = [copies.start(view, view, across(0))]

    def gate_and_up(c):
        for copy in flights[c + 1]:
            copy.wait_recv()
        for copy in gate_up[c]:
            copy.wait()

        @pl.loop(0, per_group)
        def _(e):
            x = xbuf[c].reshape(total, chunk)
            for i, w in enumerate((wg, wu)):
                product = jnp.dot(x, w[c, e], preferred_element_type=jnp.float32)
                if c == 0:
                    acc[e, i] = product
                else:
                    acc[e, i] += product

    stages = len(upper) + 2
    for t in range(count + stages - 1):
        for k in range(stages):
            c = t - k
            if not 0 <= c < count:
                continue
            for n in ((0, 1) if c == 0 else (c + 1,)):
                if k == 0:
                    gather_first(n)
                elif k < stages - 1:
                    gather_next(n, k)
            if k == stages - 1:
                gate_and_up(c)

    for copy in flights[0]:
        copy.wait_recv()
    table = xtab[...].reshape(total, LANES).astype(jnp.float32)
    lane = lax.broadcasted_iota(jnp.int32, table.shape, 1)
    for e in range(per_group):
        weight = jnp.sum(jnp.where(lane == row * per_group + e, table, 0.0), axis=1, keepdims=True)
        gate, up = acc[e, 0], acc[e, 1]
        hidden = gate / (1.0 + jnp.exp(-gate)) * up * weight
        hid[:, e * ff : (e + 1) * ff] = hidden.astype(hid.dtype)

    tile = max(w for w in (LANES, 2 * LANES) if chunk % w == 0)
    spread = (2,) * bits
    returns = [None] * count

    def project(c):
        down[c].wait()

        @pl.loop(0, chunk // tile)
        def _(i):
            span = pl.ds(pl.multiple_of(i * tile, tile), tile)
            w = wd[c, :, :, span].reshape(per_group * ff, tile)
            product = jnp.dot(hid[...], w, preferred_element_type=jnp.float32)
            part[(c,) + (slice(None),) * (bits + 1) + (span,)] = (
                product.astype(part.dtype).reshape(spread + (rows, tile))
            )

        view = part.at[c].at[at({0: 1 - mine[0]}, slice(None))]
        returns[c] = [copies.start(view, rcore.at[c], across(0))]

    def reduce_stage(c, k):
        for copy in returns[c]:
            copy.wait_recv()
        chunk_part = part.at[c]
        if k == 0:
            index = at({0: mine[0]}, slice(None))
            both = chunk_part[index].astype(jnp.float32) + rcore[c].astype(jnp.float32)
            chunk_part[index] = both.astype(part.dtype)
        else:
            for p, (offset, width) in enumerate(parts):
                fixed = {i: mine[i] for i in [0] + orders[p][:k]}
                index = at(fixed, pl.ds(offset, width))
                both = chunk_part[index].astype(jnp.float32) + arrived(c, k - 1, p)[...].astype(jnp.float32)
                if k < len(upper):
                    chunk_part[index] = both.astype(part.dtype)
                else:
                    p3[c, :, :, offset : offset + width] = (
                        both.reshape(n_col, tok_count, width).astype(p3.dtype)
                    )
        returns[c] = []
        if k < len(upper):
            for p, (offset, width) in enumerate(parts):
                fixed = {i: mine[i] for i in [0] + orders[p][:k]}
                fixed[orders[p][k]] = 1 - mine[orders[p][k]]
                view = chunk_part.at[at(fixed, pl.ds(offset, width))]
                returns[c].append(copies.start(view, arrived(c, k, p), across(orders[p][k])))
        else:
            for j in range(1, n_col):
                returns[c].append(copies.start(p3.at[c, (col + j) % n_col], r4.at[c, j - 1], along(j)))

    def arrived(c, k, p):
        offset, width = parts[p]
        free = len(upper) - 1 - k
        return rstage[k].at[(c,) + (slice(None),) * (free + 1) + (pl.ds(offset, width),)]

    def finish(c):
        for copy in returns[c]:
            copy.wait_recv()
        whole = p3[c, col].astype(jnp.float32)
        for j in range(1, n_col):
            whole = whole + r4[c, j - 1].astype(jnp.float32)
        out_ref[:, c * chunk : (c + 1) * chunk] = whole.astype(out_ref.dtype)

    last = len(upper) + 2
    for t in range(count + last):
        for k in range(last + 1):
            c = t - k
            if not 0 <= c < count:
                continue
            if k == 0:
                project(c)
            elif k < last:
                reduce_stage(c, k - 1)
            else:
                finish(c)

    for copy in copies.sent:
        copy.wait_send()


def local(n_row, n_col, tokens, router_logits, expert_ids, w_gate, w_up, w_down):
    tok_count, width = tokens.shape
    per_group, _, ff = w_gate.shape
    rows = n_col * tok_count
    bits = n_row.bit_length() - 1
    count, chunk = column_chunks(width, CHUNKS)
    spread = (2,) * bits
    b16, f32 = jnp.bfloat16, jnp.float32
    upper = bits - 1
    sends = (n_col - 1) + upper + 1 + count * 2 * ((n_col - 1) + upper * upper + 1)
    scratch = [
        pltpu.VMEM(tokens.shape, b16),
        pltpu.VMEM(router_logits.shape, f32),
        pltpu.VMEM(expert_ids.shape, jnp.int32),
        pltpu.VMEM((tok_count, LANES), b16),
        pltpu.VMEM((count, per_group, chunk, ff), b16),
        pltpu.VMEM((count, per_group, chunk, ff), b16),
        pltpu.VMEM((count, per_group, ff, chunk), b16),
        pltpu.VMEM((count, n_col, tok_count, chunk), b16),
        pltpu.VMEM((n_col, tok_count, LANES), b16),
        pltpu.VMEM((count,) + spread + (rows, chunk), b16),
        pltpu.VMEM(spread + (rows, LANES), b16),
        pltpu.VMEM((per_group, 2, n_row * rows, ff), f32),
        pltpu.VMEM((n_row * rows, per_group * ff), b16),
        pltpu.VMEM((count,) + spread + (rows, chunk), b16),
        pltpu.VMEM((count,) + spread[1:] + (rows, chunk), b16),
        [pltpu.VMEM((count,) + (2,) * (upper - 1 - k) + (rows, chunk), b16) for k in range(upper)],
        pltpu.VMEM((count, n_col, tok_count, chunk), b16),
        pltpu.VMEM((count, n_col - 1, tok_count, chunk), b16),
        pltpu.SemaphoreType.DMA((3,)),
        pltpu.SemaphoreType.DMA((3, count)),
        pltpu.SemaphoreType.DMA((sends,)),
        pltpu.SemaphoreType.DMA((sends,)),
    ]
    return pl.pallas_call(
        functools.partial(kernel, n_row, n_col, count, chunk),
        out_shape=jax.ShapeDtypeStruct(tokens.shape, b16),
        in_specs=[pl.BlockSpec(memory_space=pl.ANY)] * 6,
        out_specs=pl.BlockSpec(memory_space=pltpu.VMEM),
        scratch_shapes=scratch,
        compiler_params=pltpu.CompilerParams(
            collective_id=0, has_side_effects=True, vmem_limit_bytes=67043328
        ),
    )(tokens, router_logits, expert_ids, w_gate, w_up, w_down)


CHUNKS = 4


def solution(mesh):
    in_specs = (
        P(("row", "col"), None),
        P(("row", "col"), None),
        P(("row", "col"), None),
        P("row", None, "col"),
        P("row", None, "col"),
        P("row", "col", None),
    )
    body = functools.partial(local, mesh.shape["row"], mesh.shape["col"])
    return jax.shard_map(
        body, mesh=mesh, in_specs=in_specs, out_specs=P(("row", "col"), None), check_vma=False
    )
```

```python
import functools
import jax
import jax.numpy as jnp
from jax import lax
from jax.experimental import pallas as pl
from jax.experimental.pallas import tpu as pltpu
from jax.sharding import PartitionSpec as P

MESH = pl.DeviceIdType.MESH
LANES = 128


def column_chunks(width, wanted):
    tiles = width // LANES
    count = max(n for n in range(1, wanted + 1) if tiles % n == 0)
    return count, width // count


def split_parts(width, count):
    tiles = width // LANES
    edges = [tiles * i // count * LANES for i in range(count + 1)]
    return [(edges[i], edges[i + 1] - edges[i]) for i in range(count)]


def plan(count, lags, stages):
    step = (lags[-1] - lags[0]) / (len(lags) - 1)
    lags = list(lags) + [lags[-1] + step * (i + 1) for i in range(stages - len(lags))]
    return sorted(((c, k) for c in range(count) for k in range(stages)), key=lambda e: (e[0] + lags[e[1]], e[1]))


class Copies:
    def __init__(self, send_sems, recv_sems):
        self.send_sems, self.recv_sems, self.used, self.sent = send_sems, recv_sems, 0, []

    def start(self, src, dst, target):
        n = self.used
        self.used += 1
        copy = pltpu.make_async_remote_copy(
            src_ref=src,
            dst_ref=dst,
            send_sem=self.send_sems.at[n],
            recv_sem=self.recv_sems.at[n],
            device_id=target,
            device_id_type=MESH,
        )
        copy.start()
        self.sent.append(copy)
        return copy


def kernel(
    n_row, n_col, count, chunk,
    tokens_hbm, logits_hbm, ids_hbm, gate_hbm, up_hbm, down_hbm,
    out_ref,
    tok, logits, ids, table_own, wg, wu, wd,
    zbuf, ztab, xbuf, xtab, acc, hid, part, rcore, rstage, p3, r4,
    small_sems, weight_sems, send_sems, recv_sems,
):
    bits = n_row.bit_length() - 1
    upper = list(range(1, bits))
    tok_count = tok.shape[0]
    rows = n_col * tok_count
    per_group, ff = wg.shape[1], wg.shape[3]
    total = n_row * rows
    experts = logits.shape[1]

    row, col = lax.axis_index("row"), lax.axis_index("col")
    mine = [(row // 2**i) % 2 for i in range(bits)]

    def across(i):
        return {"row": row + 2**i * (1 - 2 * mine[i]), "col": col}

    def along(j):
        return {"row": row, "col": (col + j) % n_col}

    def at(fixed, *tail):
        return tuple(fixed.get(i, slice(None)) for i in reversed(range(bits))) + (slice(None),) + tail

    orders = [upper[p:] + upper[:p] for p in range(len(upper))]

    small = [
        pltpu.make_async_copy(src, dst, small_sems.at[i])
        for i, (src, dst) in enumerate(((tokens_hbm, tok), (logits_hbm, logits), (ids_hbm, ids)))
    ]
    for copy in small:
        copy.start()
    gate_up, down = [], []
    for c in range(count):
        span = pl.ds(c * chunk, chunk)
        pair = [
            pltpu.make_async_copy(gate_hbm.at[:, span, :], wg.at[c], weight_sems.at[0, c]),
            pltpu.make_async_copy(up_hbm.at[:, span, :], wu.at[c], weight_sems.at[1, c]),
        ]
        gate_up.append(pair)
    for c in range(count):
        copy = pltpu.make_async_copy(down_hbm.at[:, :, pl.ds(c * chunk, chunk)], wd.at[c], weight_sems.at[2, c])
        down.append(copy)

    barrier = pltpu.get_barrier_semaphore()
    peers = [across(i) for i in range(bits)] + [along(j) for j in range(1, n_col)]
    for peer in peers:
        pl.semaphore_signal(barrier, inc=1, device_id=peer, device_id_type=MESH)

    small[0].wait()

    pl.semaphore_wait(barrier, len(peers))
    copies = Copies(send_sems, recv_sems)

    parts = split_parts(chunk, len(upper))
    pieces = [(table_own, ztab, xtab, [(0, LANES)])]
    pieces += [(tok.at[:, pl.ds(c * chunk, chunk)], zbuf.at[c], xbuf.at[c], parts) for c in range(count)]
    flights = [None] * len(pieces)

    def send_own(n):
        own, z, _, _ = pieces[n]
        flights[n] = [copies.start(own, z.at[col], along(j)) for j in range(1, n_col)]
        z[col] = own[...]

    def start_all(started):
        for copy in started:
            copy.start()

    stages = len(upper) + 2
    events = plan(count, GATHER_LAGS, stages + 3)
    ahead = next(i for i, e in enumerate(events) if e[1] == 3)
    for c, k in events[:ahead]:
        if k == 0:
            send_own(c + 1)
        else:
            start_all(gate_up[c] if k == 1 else [down[c]])

    small[1].wait()
    small[2].wait()
    scores, named = logits[...], ids[...]
    lane = lax.broadcasted_iota(jnp.int32, scores.shape, 1)
    marks = jnp.zeros(scores.shape, jnp.float32)
    for k in range(named.shape[1]):
        marks = marks + jnp.where(named[:, k : k + 1] == lane, 1.0, 0.0)
    chosen = marks > 0.5
    top = jnp.max(jnp.where(chosen, scores, -jnp.inf), axis=1, keepdims=True)
    weight = jnp.where(chosen, jnp.exp(jnp.where(chosen, scores, top) - top), 0.0)
    weight = weight / jnp.sum(weight, axis=1, keepdims=True)
    table_own[...] = jnp.zeros(table_own.shape, table_own.dtype)
    table_own[:, :experts] = weight.astype(table_own.dtype)
    send_own(0)

    def gather_first(n):
        own, z, x, spans = pieces[n]
        for copy in flights[n]:
            copy.wait_recv()
        block = z[...].astype(jnp.float32).reshape(rows, z.shape[-1]).astype(x.dtype)
        x[at({i: mine[i] for i in range(bits)}, slice(None))] = block
        gather_stage(n, 0)

    def gather_stage(n, k):
        _, _, x, spans = pieces[n]
        flights[n] = []
        for p, (offset, width) in enumerate(spans):
            done = orders[p][:k]
            fixed = {i: mine[i] for i in range(bits) if i not in done}
            view = x.at[at(fixed, pl.ds(offset, width))]
            flights[n].append(copies.start(view, view, across(orders[p][k])))

    def gather_next(n, k):
        for copy in flights[n]:
            copy.wait_recv()
        if k < len(upper):
            gather_stage(n, k)
        else:
            _, _, x, _ = pieces[n]
            view = x.at[at({0: mine[0]}, slice(None))]
            flights[n] = [copies.start(view, view, across(0))]

    def gate_and_up(c):
        for copy in flights[c + 1]:
            copy.wait_recv()
        for copy in gate_up[c]:
            copy.wait()

        @pl.loop(0, per_group)
        def _(e):
            x = xbuf[c].reshape(total, chunk)
            for i, w in enumerate((wg, wu)):
                product = jnp.dot(x, w[c, e], preferred_element_type=jnp.float32)
                if c == 0:
                    acc[e, i] = product
                else:
                    acc[e, i] += product

    for c, k in events[ahead:]:
        if k == 0:
            send_own(c + 1)
            continue
        if k in (1, 2):
            start_all(gate_up[c] if k == 1 else [down[c]])
            continue
        k -= 3
        for n in (0, c + 1) if c == count // 2 else (c + 1,):
            if k == 0:
                gather_first(n)
            elif k < stages - 1:
                gather_next(n, k)
        if k == stages - 1:
            gate_and_up(c)

    for copy in flights[0]:
        copy.wait_recv()
    table = xtab[...].reshape(total, LANES).astype(jnp.float32)
    lane = lax.broadcasted_iota(jnp.int32, table.shape, 1)
    for e in range(per_group):
        weight = jnp.sum(jnp.where(lane == row * per_group + e, table, 0.0), axis=1, keepdims=True)
        gate, up = acc[e, 0], acc[e, 1]
        hidden = gate / (1.0 + jnp.exp(-gate)) * up * weight
        hid[:, e * ff : (e + 1) * ff] = hidden.astype(hid.dtype)

    tile = max(w for w in (LANES, 2 * LANES) if chunk % w == 0)
    spread = (2,) * bits
    returns = [None] * count

    def project(c):
        down[c].wait()

        @pl.loop(0, chunk // tile)
        def _(i):
            span = pl.ds(pl.multiple_of(i * tile, tile), tile)
            w = wd[c, :, :, span].reshape(per_group * ff, tile)
            product = jnp.dot(hid[...], w, preferred_element_type=jnp.float32)
            part[(c,) + (slice(None),) * (bits + 1) + (span,)] = (
                product.astype(part.dtype).reshape(spread + (rows, tile))
            )

        view = part.at[c].at[at({0: 1 - mine[0]}, slice(None))]
        returns[c] = [copies.start(view, rcore.at[c], across(0))]

    def reduce_stage(c, k):
        for copy in returns[c]:
            copy.wait_recv()
        chunk_part = part.at[c]
        if k == 0:
            index = at({0: mine[0]}, slice(None))
            both = chunk_part[index].astype(jnp.float32) + rcore[c].astype(jnp.float32)
            chunk_part[index] = both.astype(part.dtype)
        else:
            for p, (offset, width) in enumerate(parts):
                fixed = {i: mine[i] for i in [0] + orders[p][:k]}
                index = at(fixed, pl.ds(offset, width))
                both = chunk_part[index].astype(jnp.float32) + arrived(c, k - 1, p)[...].astype(jnp.float32)
                if k < len(upper):
                    chunk_part[index] = both.astype(part.dtype)
                else:
                    p3[c, :, :, offset : offset + width] = (
                        both.reshape(n_col, tok_count, width).astype(p3.dtype)
                    )
        returns[c] = []
        if k < len(upper):
            for p, (offset, width) in enumerate(parts):
                fixed = {i: mine[i] for i in [0] + orders[p][:k]}
                fixed[orders[p][k]] = 1 - mine[orders[p][k]]
                view = chunk_part.at[at(fixed, pl.ds(offset, width))]
                returns[c].append(copies.start(view, arrived(c, k, p), across(orders[p][k])))
        else:
            for j in range(1, n_col):
                returns[c].append(copies.start(p3.at[c, (col + j) % n_col], r4.at[c, j - 1], along(j)))

    def arrived(c, k, p):
        offset, width = parts[p]
        free = len(upper) - 1 - k
        return rstage[k].at[(c,) + (slice(None),) * (free + 1) + (pl.ds(offset, width),)]

    def finish(c):
        for copy in returns[c]:
            copy.wait_recv()
        whole = p3[c, col].astype(jnp.float32)
        for j in range(1, n_col):
            whole = whole + r4[c, j - 1].astype(jnp.float32)
        out_ref[:, c * chunk : (c + 1) * chunk] = whole.astype(out_ref.dtype)

    last = len(upper) + 2
    for c, k in plan(count, RETURN_LAGS, last + 1):
        if k == 0:
            project(c)
        elif k < last:
            reduce_stage(c, k - 1)
        else:
            finish(c)

    for copy in copies.sent:
        copy.wait_send()


def local(n_row, n_col, tokens, router_logits, expert_ids, w_gate, w_up, w_down):
    tok_count, width = tokens.shape
    per_group, _, ff = w_gate.shape
    rows = n_col * tok_count
    bits = n_row.bit_length() - 1
    count, chunk = column_chunks(width, CHUNKS)
    spread = (2,) * bits
    b16, f32 = jnp.bfloat16, jnp.float32
    upper = bits - 1
    sends = (n_col - 1) + upper + 1 + count * 2 * ((n_col - 1) + upper * upper + 1)
    scratch = [
        pltpu.VMEM(tokens.shape, b16),
        pltpu.VMEM(router_logits.shape, f32),
        pltpu.VMEM(expert_ids.shape, jnp.int32),
        pltpu.VMEM((tok_count, LANES), b16),
        pltpu.VMEM((count, per_group, chunk, ff), b16),
        pltpu.VMEM((count, per_group, chunk, ff), b16),
        pltpu.VMEM((count, per_group, ff, chunk), b16),
        pltpu.VMEM((count, n_col, tok_count, chunk), b16),
        pltpu.VMEM((n_col, tok_count, LANES), b16),
        pltpu.VMEM((count,) + spread + (rows, chunk), b16),
        pltpu.VMEM(spread + (rows, LANES), b16),
        pltpu.VMEM((per_group, 2, n_row * rows, ff), f32),
        pltpu.VMEM((n_row * rows, per_group * ff), b16),
        pltpu.VMEM((count,) + spread + (rows, chunk), b16),
        pltpu.VMEM((count,) + spread[1:] + (rows, chunk), b16),
        [pltpu.VMEM((count,) + (2,) * (upper - 1 - k) + (rows, chunk), b16) for k in range(upper)],
        pltpu.VMEM((count, n_col, tok_count, chunk), b16),
        pltpu.VMEM((count, n_col - 1, tok_count, chunk), b16),
        pltpu.SemaphoreType.DMA((3,)),
        pltpu.SemaphoreType.DMA((3, count)),
        pltpu.SemaphoreType.DMA((sends,)),
        pltpu.SemaphoreType.DMA((sends,)),
    ]
    return pl.pallas_call(
        functools.partial(kernel, n_row, n_col, count, chunk),
        out_shape=jax.ShapeDtypeStruct(tokens.shape, b16),
        in_specs=[pl.BlockSpec(memory_space=pl.ANY)] * 6,
        out_specs=pl.BlockSpec(memory_space=pltpu.VMEM),
        scratch_shapes=scratch,
        compiler_params=pltpu.CompilerParams(
            collective_id=0, has_side_effects=True, vmem_limit_bytes=67043328
        ),
    )(tokens, router_logits, expert_ids, w_gate, w_up, w_down)


CHUNKS = 4
GATHER_LAGS = (-1.5, -1.2, 1.8, 0, 1, 2, 3)
RETURN_LAGS = (0, 1, 2, 3, 4)


def solution(mesh):
    in_specs = (
        P(("row", "col"), None),
        P(("row", "col"), None),
        P(("row", "col"), None),
        P("row", None, "col"),
        P("row", None, "col"),
        P("row", "col", None),
    )
    body = functools.partial(local, mesh.shape["row"], mesh.shape["col"])
    return jax.shard_map(
        body, mesh=mesh, in_specs=in_specs, out_specs=P(("row", "col"), None), check_vma=False
    )
```
